32 devices in a mesh: row: 4 (over y, x), col: 4 (over z), trial: 2 (over core).
Axes of the slice: x: 2, y: 2, z: 4, core: 2. Of those that a mesh axis runs over, the one named last changes fastest.
Arguments:
- pair_rows: bfloat16 [192, 96, 128], P(('trial', 'row'), 'col'), parts along dimension 0, may hold values from -6 to 6
- left_weight: bfloat16 [256, 128], P('trial'), parts along dimension 0, may hold values from -0.5 to 0.5
- right_weight: bfloat16 [256, 128], P('trial'), parts along dimension 0, may hold values from -0.5 to 0.5
- left_gate: bfloat16 [256, 128], P('trial'), parts along dimension 0, may hold values from -0.5 to 0.5
- right_gate: bfloat16 [256, 128], P('trial'), parts along dimension 0, may hold values from -0.5 to 0.5
- mid_gain: float32 [128], replicated, may hold values from 0.25 to 1.75
- out_weight: bfloat16 [256, 128], P('trial'), parts along dimension 0, may hold values from -0.5 to 0.5
- out_gate: bfloat16 [256, 128], P('trial'), parts along dimension 0, may hold values from -0.5 to 0.5
Outputs:
- pair_change: bfloat16 [192, 96, 128], P(('trial', 'row'), 'col'), parts along dimension 0
The draws below stay inside these ranges and needn't reach their ends.
There are 2 independent parts, one for each index of `trial`. The reference program is written for one: setup_inputs(seed, part) draws one part's arguments, and reference() takes and returns one part's arrays. A program takes and returns all parts, laid end to end along the dimension named above; an argument that names none is the same for every part. Nothing has to cross between parts.
All inputs are finite; a program needn't handle non-finite values.
Results may differ from the reference program's by a relative error of at most 0.015.
Values may be sent and summed in bfloat16 or wider, within the bound.
No kernel may reach another device: no remote copies, remote signals or barrier semaphores. Data moves between devices by JAX's collectives and lax.ppermute only.
A program may use at most 64 MiB of HBM per device.

```python
import jax
import jax.numpy as jnp
from jax import lax

RESIDUES = 96
PAIR_WIDTH = 128
MIX_WIDTH = 128


def shard_levels(stream_key, shape, split, least, top_value):
    def one(axis_at, blocks):
        draws = jax.random.uniform(jax.random.fold_in(jax.random.fold_in(stream_key, 6), axis_at), (blocks,), jnp.float32, least / len(split), top_value / len(split))
        return jnp.repeat(jnp.exp(draws), shape[axis_at] // blocks).reshape((-1,) + (1,) * (len(shape) - axis_at - 1))

    factor_of = one(*split[0])
    for cut in split[1:]:
        factor_of = factor_of * one(*cut)
    return factor_of


def normal_values(own_key, extent, spread, bound, cuts=(), dtype=jnp.bfloat16):
    values = spread * jax.random.normal(own_key, extent, jnp.float32)
    if cuts:
        values = values * shard_levels(own_key, extent, cuts, -0.22, 0.18)
    return jnp.clip(values, -bound, bound).astype(dtype)


def setup_inputs(seed: int = 0, part: int = 0) -> dict:
    key_of = jax.random.split(jax.random.key(seed), 9)
    own_keys = jax.random.split(jax.random.fold_in(key_of[8], part), 9)
    return {
        "pair_rows": normal_values(own_keys[0], (RESIDUES, RESIDUES, PAIR_WIDTH), 1.0, 6.0, ((0, 4), (1, 4))),
        "left_weight": normal_values(own_keys[1], (PAIR_WIDTH, MIX_WIDTH), PAIR_WIDTH ** -0.5, 0.5),
        "right_weight": normal_values(own_keys[2], (PAIR_WIDTH, MIX_WIDTH), PAIR_WIDTH ** -0.5, 0.5),
        "left_gate": normal_values(own_keys[3], (PAIR_WIDTH, MIX_WIDTH), PAIR_WIDTH ** -0.5, 0.5),
        "right_gate": normal_values(own_keys[4], (PAIR_WIDTH, MIX_WIDTH), PAIR_WIDTH ** -0.5, 0.5),
        "mid_gain": jnp.clip(1.0 + 0.15 * jax.random.normal(key_of[5], (MIX_WIDTH,), jnp.float32), 0.25, 1.75),
        "out_weight": normal_values(own_keys[6], (MIX_WIDTH, PAIR_WIDTH), MIX_WIDTH ** -0.5, 0.5),
        "out_gate": normal_values(own_keys[7], (PAIR_WIDTH, PAIR_WIDTH), PAIR_WIDTH ** -0.5, 0.5),
    }


def norm_channels(values, channel_gain):
    centred = values - lax.optimization_barrier(jnp.mean(values, axis=-1, keepdims=True))
    return centred * lax.rsqrt(lax.optimization_barrier(jnp.mean(centred * centred, axis=-1, keepdims=True)) + 1e-05) * channel_gain

def both_factors(pair_in, left_weight, right_weight, left_gate, right_gate):
    ready = pair_in
    left = jnp.einsum('ijc,cd->ijd', ready.astype(jnp.float32), left_weight.astype(jnp.float32))
    left = left * jax.nn.sigmoid(jnp.einsum('ijc,cd->ijd', ready.astype(jnp.float32), left_gate.astype(jnp.float32)))
    right = jnp.einsum('ijc,cd->ijd', ready.astype(jnp.float32), right_weight.astype(jnp.float32))
    right = right * jax.nn.sigmoid(jnp.einsum('ijc,cd->ijd', ready.astype(jnp.float32), right_gate.astype(jnp.float32)))
    return (ready, left.astype(jnp.bfloat16), right.astype(jnp.bfloat16))

def close_update(mixed, ready, mid_gain, out_weight, out_gate):
    scaled = norm_channels(mixed.astype(jnp.float32), mid_gain).astype(jnp.bfloat16)
    scaled = lax.optimization_barrier(scaled)
    gate = jax.nn.sigmoid(jnp.einsum('ijc,cd->ijd', ready.astype(jnp.float32), out_gate.astype(jnp.float32)))
    return (jnp.einsum('ijd,dc->ijc', scaled.astype(jnp.float32), out_weight.astype(jnp.float32)) * gate).astype(jnp.bfloat16)

def reference(pair_rows, left_weight, right_weight, left_gate, right_gate, mid_gain, out_weight, out_gate):
    ready, left, right = both_factors(pair_rows, left_weight, right_weight, left_gate, right_gate)
    left, right = lax.optimization_barrier((left, right))

    def one_channel(pair_of):
        return (jnp.dot(pair_of[0].T, pair_of[1], preferred_element_type=jnp.float32) * RESIDUES ** (-0.5)).astype(jnp.bfloat16)
    mixed = jnp.moveaxis(lax.map(one_channel, (jnp.moveaxis(left, -1, 0), jnp.moveaxis(right, -1, 0))), 0, -1)
    mixed = lax.optimization_barrier(mixed)
    return close_update(mixed, ready, mid_gain, out_weight, out_gate)
```

```python
import functools

import jax
import jax.numpy as jnp
from jax import lax
from jax.experimental import pallas as pl
from jax.experimental.pallas import tpu as pltpu
from jax.sharding import PartitionSpec as P

F32 = jnp.float32
BF16 = jnp.bfloat16


def logistic(x):
    return 0.5 + 0.5 * jnp.tanh(0.5 * x)


def pick(a, b, n):
    return a ^ b if n & (n - 1) == 0 else (a + b) % n


def factor_kernel(x_ref, w_ref, g_ref, out_ref):
    both = jnp.concatenate([w_ref[...], g_ref[...]], axis=1)
    width = w_ref.shape[1]
    prod = jnp.dot(x_ref[...], both, preferred_element_type=F32)
    out_ref[...] = (prod[:, :width] * logistic(prod[:, width:])).astype(out_ref.dtype)


def gate_kernel(x_ref, g_ref, out_ref):
    out_ref[...] = logistic(jnp.dot(x_ref[...], g_ref[...], preferred_element_type=F32))


def close_kernel(n, lines, parts, *refs):
    where_ref = refs[0]
    lefts = refs[1 : 1 + lines]
    rights = refs[1 + lines : 1 + lines + parts]
    gate_ref, gain_ref, weight_ref, out_ref, left_f, right_f, acc = refs[1 + lines + parts :]
    k_count, j_count, width = lefts[0].shape
    group = 4
    groups = j_count // group
    for m in range(parts):
        right_f[where_ref[lines * 2 + m]] = rights[m][...].astype(F32)
    acc[...] = jnp.zeros_like(acc)
    chunk = 8
    for u in range(lines):
        left_f[...] = lefts[u][...].astype(F32)
        source = where_ref[u]
        base = where_ref[lines + u] * j_count

        def one_group(g, _):
            at = g * group

            def some_k(t, sums):
                sums = list(sums)
                for kk in range(chunk):
                    k = t * chunk + kk
                    row = right_f[source, k]
                    for ii in range(group):
                        sums[ii] = sums[ii] + left_f[k, pl.ds(at + ii, 1), :] * row
                return tuple(sums)

            sums = tuple(acc[base + at + ii] for ii in range(group))
            sums = lax.fori_loop(0, k_count // chunk, some_k, sums)
            for ii in range(group):
                acc[base + at + ii] = sums[ii]
            return 0

        lax.fori_loop(0, groups, one_group, 0)
    mixed = (acc[...] * n ** (-0.5)).astype(BF16).astype(F32)
    centred = mixed - jnp.mean(mixed, axis=-1, keepdims=True)
    var = jnp.mean(centred * centred, axis=-1, keepdims=True)
    scaled = centred * lax.rsqrt(var + 1e-05) * gain_ref[...]
    scaled = scaled.reshape(-1, width).astype(BF16)
    prod = jnp.dot(scaled, weight_ref[...], preferred_element_type=F32)
    out_ref[...] = (prod * gate_ref[...]).astype(out_ref.dtype)


VMEM = pl.BlockSpec(memory_space=pltpu.VMEM)
SMEM = pl.BlockSpec(memory_space=pltpu.SMEM)


def per_device(
    pair_rows, left_weight, right_weight, left_gate, right_gate, mid_gain, out_weight, out_gate
):
    k_count, j_count, width = pair_rows.shape
    mix = left_weight.shape[1]
    rows, cols = lax.axis_size("row"), lax.axis_size("col")
    n = k_count * rows
    per_row = cols // rows
    flat = pair_rows.reshape(k_count * j_count, width)

    def factor(weight, gate):
        out = pl.pallas_call(
            factor_kernel,
            out_shape=jax.ShapeDtypeStruct((k_count * j_count, mix), BF16),
            in_specs=[VMEM] * 3,
            out_specs=VMEM,
        )(flat, weight, gate)
        return out.reshape(k_count, j_count, mix)

    left = factor(left_weight, left_gate)
    both = ("row", "col")

    def source_of(r, c, u):
        return pick(pick(c, r * per_row, cols), u, cols)

    lefts = []
    for u in range(cols):
        moves = []
        for r in range(rows):
            for c in range(cols):
                e = source_of(r, c, u)
                moves.append((e // per_row * cols + r * per_row + e % per_row, r * cols + c))
        lefts.append(lax.ppermute(left, both, moves))
    right = factor(right_weight, right_gate)
    rights = [right]
    for m in range(1, rows):
        rights.append(lax.ppermute(right, "row", [(pick(r, m, rows), r) for r in range(rows)]))
    gate = pl.pallas_call(
        gate_kernel,
        out_shape=jax.ShapeDtypeStruct((k_count * j_count, width), F32),
        in_specs=[VMEM] * 2,
        out_specs=VMEM,
    )(flat, out_gate)
    r, c = lax.axis_index("row"), lax.axis_index("col")
    sources = [source_of(r, c, u) for u in range(cols)]
    where = jnp.stack(
        [e // per_row for e in sources]
        + [e % per_row for e in sources]
        + [pick(r, m, rows) for m in range(rows)]
    ).astype(jnp.int32)

    out = pl.pallas_call(
        functools.partial(close_kernel, n, cols, rows),
        out_shape=jax.ShapeDtypeStruct((k_count * j_count, width), BF16),
        in_specs=[SMEM] + [VMEM] * (cols + rows + 3),
        out_specs=VMEM,
        scratch_shapes=[
            pltpu.VMEM((k_count, j_count, mix), F32),
            pltpu.VMEM((rows, k_count, j_count, mix), F32),
            pltpu.VMEM((k_count, j_count, mix), F32),
        ],
    )(where, *lefts, *rights, gate, mid_gain.reshape(1, -1), out_weight)
    return out.reshape(k_count, j_count, width)


def solution(mesh):
    placed = (
        P(("trial", "row"), "col", None),
        P("trial", None),
        P("trial", None),
        P("trial", None),
        P("trial", None),
        P(),
        P("trial", None),
        P("trial", None),
    )
    return jax.shard_map(
        per_device,
        mesh=mesh,
        in_specs=placed,
        out_specs=P(("trial", "row"), "col", None),
        check_vma=False,
    )
```

```python
import functools

import jax
import jax.numpy as jnp
from jax import lax
from jax.experimental import pallas as pl
from jax.experimental.pallas import tpu as pltpu
from jax.sharding import PartitionSpec as P

F32 = jnp.float32
BF16 = jnp.bfloat16
NEAR_BYTES = 4 * 2**20


def logistic(x):
    return 0.5 + 0.5 * jnp.tanh(0.5 * x)


def pick(a, b, n):
    return a ^ b if n & (n - 1) == 0 else (a + b) % n


def factor(x, weight, gate):
    width = weight.shape[1]
    both = jnp.concatenate([weight, gate], axis=1)
    prod = jnp.dot(x, both, preferred_element_type=F32)
    return (prod[:, :width] * logistic(prod[:, width:])).astype(BF16).astype(F32)


def right_kernel(x_ref, weight_ref, gate_ref, out_gate_ref, *refs):
    right_ref, out_ref = refs[-2:]
    rows = right_ref.shape[0]
    me = lax.axis_index("row")
    out_ref[...] = logistic(jnp.dot(x_ref[...], out_gate_ref[...], preferred_element_type=F32))
    for m, each in enumerate((x_ref,) + refs[:-2]):
        right = factor(each[...], weight_ref[...], gate_ref[...])
        right_ref[pick(me, m, rows)] = right.reshape(right_ref.shape[1:])


def add_line(u, x_ref, weight_ref, gate_ref, right_ref, acc_ref, left_f):
    left_f[...] = factor(x_ref[...], weight_ref[...], gate_ref[...]).reshape(left_f.shape)
    k_count, j_count, _ = left_f.shape
    rows, cols = lax.axis_size("row"), lax.axis_size("col")
    e = pick(lax.axis_index("col"), u, cols)
    source = e // (cols // rows)
    base = e % (cols // rows) * j_count
    group, chunk = 4, 8

    def one_group(g, _):
        at = g * group

        def some_k(t, sums):
            sums = list(sums)
            for kk in range(chunk):
                k = t * chunk + kk
                row = right_ref[source, k]
                for ii in range(group):
                    sums[ii] = sums[ii] + left_f[k, pl.ds(at + ii, 1), :] * row
            return tuple(sums)

        sums = tuple(acc_ref[base + at + ii] for ii in range(group))
        sums = lax.fori_loop(0, k_count // chunk, some_k, sums)
        for ii in range(group):
            acc_ref[base + at + ii] = sums[ii]
        return 0

    lax.fori_loop(0, j_count // group, one_group, 0)


def first_kernel(u, x_ref, weight_ref, gate_ref, right_ref, acc_ref, left_f):
    acc_ref[...] = jnp.zeros_like(acc_ref)
    add_line(u, x_ref, weight_ref, gate_ref, right_ref, acc_ref, left_f)


def next_kernel(u, x_ref, weight_ref, gate_ref, right_ref, old_ref, acc_ref, left_f):
    del old_ref
    add_line(u, x_ref, weight_ref, gate_ref, right_ref, acc_ref, left_f)


def last_kernel(
    u, n, x_ref, weight_ref, gate_ref, right_ref, old_ref,
    out_gate_ref, gain_ref, out_weight_ref, out_ref, left_f,
):
    add_line(u, x_ref, weight_ref, gate_ref, right_ref, old_ref, left_f)
    mixed = (old_ref[...] * n ** (-0.5)).astype(BF16).astype(F32)
    centred = mixed - jnp.mean(mixed, axis=-1, keepdims=True)
    var = jnp.mean(centred * centred, axis=-1, keepdims=True)
    scaled = centred * lax.rsqrt(var + 1e-05) * gain_ref[...]
    scaled = scaled.reshape(-1, scaled.shape[-1]).astype(BF16)
    prod = jnp.dot(scaled, out_weight_ref[...], preferred_element_type=F32)
    out_ref[...] = (prod * out_gate_ref[...]).astype(out_ref.dtype)


VMEM = pl.BlockSpec(memory_space=pltpu.VMEM)


def call(kernel, near, outs, scratch, *args, aliases={}):
    if near:
        args = [pltpu.with_memory_space_constraint(each, pltpu.VMEM) for each in args]
    return pl.pallas_call(
        kernel,
        out_shape=outs,
        in_specs=[VMEM] * len(args),
        out_specs=jax.tree.map(lambda _: VMEM, outs),
        input_output_aliases=aliases,
        scratch_shapes=[pltpu.VMEM(each, F32) for each in scratch],
    )(*args)


def update(
    pair_rows, left_weight, right_weight, left_gate, right_gate, mid_gain, out_weight, out_gate
):
    k_count, j_count, width = pair_rows.shape
    mix = left_weight.shape[1]
    rows, cols = lax.axis_size("row"), lax.axis_size("col")
    n = k_count * rows
    per_row = cols // rows
    flat = pair_rows.reshape(k_count * j_count, width)
    block = (k_count, j_count, mix)
    rights = []
    for m in range(1, rows):
        rights.append(lax.ppermute(flat, "row", [(pick(s, m, rows), s) for s in range(rows)]))
    lefts = []
    for u in range(cols):
        moves = []
        for rr in range(rows):
            for cc in range(cols):
                e = pick(cc, u, cols)
                moves.append((e // per_row * cols + rr * per_row + e % per_row, rr * cols + cc))
        lefts.append(lax.ppermute(flat, ("row", "col"), moves))
    one = k_count * j_count * max(mix, width)
    near = one * (4 * (rows + 2) + 2 * (rows + cols)) <= NEAR_BYTES
    held = pltpu.VMEM if near else jax.ShapeDtypeStruct
    right, gate = call(
        right_kernel,
        near,
        (held((rows,) + block, F32), held((k_count * j_count, width), F32)),
        [], flat, right_weight, right_gate, out_gate, *rights,
    )
    total = None
    for u in range(cols):
        args = [lefts[u], left_weight, left_gate, right]
        if u == 0:
            total = call(functools.partial(first_kernel, u), near, held(block, F32), [block], *args)
        elif u < cols - 1:
            total = call(
                functools.partial(next_kernel, u), near, held(block, F32), [block],
                *args, total, aliases={4: 0},
            )
        else:
            out = call(
                functools.partial(last_kernel, u, n), near,
                jax.ShapeDtypeStruct(flat.shape, BF16), [block],
                *args, total, gate, mid_gain.reshape(1, -1), out_weight,
            )
    return out.reshape(pair_rows.shape)


def solution(mesh):
    placed = (
        P(("trial", "row"), "col", None),
        P("trial", None),
        P("trial", None),
        P("trial", None),
        P("trial", None),
        P(),
        P("trial", None),
        P("trial", None),
    )
    return jax.shard_map(
        update,
        mesh=mesh,
        in_specs=placed,
        out_specs=P(("trial", "row"), "col", None),
        check_vma=False,
    )
```

```python
import functools

import jax
import jax.numpy as jnp
from jax import lax
from jax.experimental import pallas as pl
from jax.experimental.pallas import tpu as pltpu
from jax.sharding import PartitionSpec as P

F32 = jnp.float32
BF16 = jnp.bfloat16
NEAR_BYTES = 4 * 2**20


def logistic(x):
    return 0.5 + 0.5 * jnp.tanh(0.5 * x)


def pick(a, b, n):
    return a ^ b if n & (n - 1) == 0 else (a + b) % n


def step_order(rows, cols):
    half = cols // 2
    rights = [*range(rows - 1, 0, -1)]
    lefts = [*range(half, -1, -1), *range(half + 1, cols)]
    return rights, lefts


def factor(x, both):
    width = both.shape[1] // 2
    prod = jnp.dot(x, both, preferred_element_type=F32)
    return (prod[:, :width] * logistic(prod[:, width:])).astype(BF16).astype(F32)


def right_kernel(
    x_ref, weight_ref, gate_ref, left_weight_ref, left_gate_ref, out_gate_ref, *refs
):
    right_ref, out_ref, left_both_ref = refs[-3:]
    rows = right_ref.shape[0]
    me = lax.axis_index("row")
    out_ref[...] = logistic(jnp.dot(x_ref[...], out_gate_ref[...], preferred_element_type=F32))
    left_both_ref[...] = jnp.concatenate([left_weight_ref[...], left_gate_ref[...]], axis=1)
    both = jnp.concatenate([weight_ref[...], gate_ref[...]], axis=1)
    for m, each in enumerate((x_ref,) + refs[:-3]):
        right = factor(each[...], both)
        right_ref[pick(me, m, rows)] = right.reshape(right_ref.shape[1:])


def add_line(u, x_ref, both_ref, right_ref, acc_ref, left_f):
    left_f[...] = factor(x_ref[...], both_ref[...]).reshape(left_f.shape)
    k_count, j_count, _ = left_f.shape
    rows, cols = lax.axis_size("row"), lax.axis_size("col")
    e = pick(lax.axis_index("col"), u, cols)
    source = e // (cols // rows)
    base = e % (cols // rows) * j_count
    group, chunk = 4, 8

    def one_group(g, _):
        at = g * group

        def some_k(t, sums):
            sums = list(sums)
            for kk in range(chunk):
                k = t * chunk + kk
                row = right_ref[source, k]
                for ii in range(group):
                    sums[ii] = sums[ii] + left_f[k, pl.ds(at + ii, 1), :] * row
            return tuple(sums)

        sums = tuple(acc_ref[base + at + ii] for ii in range(group))
        sums = lax.fori_loop(0, k_count // chunk, some_k, sums)
        for ii in range(group):
            acc_ref[base + at + ii] = sums[ii]
        return 0

    lax.fori_loop(0, j_count // group, one_group, 0)


def first_kernel(u, x_ref, both_ref, right_ref, acc_ref, left_f):
    acc_ref[...] = jnp.zeros_like(acc_ref)
    add_line(u, x_ref, both_ref, right_ref, acc_ref, left_f)


def next_kernel(u, x_ref, both_ref, right_ref, old_ref, acc_ref, left_f):
    del old_ref
    add_line(u, x_ref, both_ref, right_ref, acc_ref, left_f)


def last_kernel(
    u, n, x_ref, both_ref, right_ref, old_ref,
    out_gate_ref, gain_ref, out_weight_ref, out_ref, left_f,
):
    add_line(u, x_ref, both_ref, right_ref, old_ref, left_f)
    mixed = (old_ref[...] * n ** (-0.5)).astype(BF16).astype(F32)
    centred = mixed - jnp.mean(mixed, axis=-1, keepdims=True)
    var = jnp.mean(centred * centred, axis=-1, keepdims=True)
    scaled = centred * lax.rsqrt(var + 1e-05) * gain_ref[...]
    scaled = scaled.reshape(-1, scaled.shape[-1]).astype(BF16)
    prod = jnp.dot(scaled, out_weight_ref[...], preferred_element_type=F32)
    out_ref[...] = (prod * out_gate_ref[...]).astype(out_ref.dtype)


VMEM = pl.BlockSpec(memory_space=pltpu.VMEM)


def call(kernel, near, outs, scratch, *args, loose=0, aliases={}):
    if near:
        args = args[:loose] + tuple(
            pltpu.with_memory_space_constraint(each, pltpu.VMEM) for each in args[loose:]
        )
    return pl.pallas_call(
        kernel,
        out_shape=outs,
        in_specs=[VMEM] * len(args),
        out_specs=jax.tree.map(lambda _: VMEM, outs),
        input_output_aliases=aliases,
        scratch_shapes=[pltpu.VMEM(each, F32) for each in scratch],
    )(*args)


def update(
    pair_rows, left_weight, right_weight, left_gate, right_gate, mid_gain, out_weight, out_gate
):
    k_count, j_count, width = pair_rows.shape
    mix = left_weight.shape[1]
    rows, cols = lax.axis_size("row"), lax.axis_size("col")
    n = k_count * rows
    per_row = cols // rows
    flat = pair_rows.reshape(k_count * j_count, width)
    block = (k_count, j_count, mix)
    rights = []
    for m in range(1, rows):
        rights.append(lax.ppermute(flat, "row", [(pick(s, m, rows), s) for s in range(rows)]))
    lefts = []
    for u in range(cols):
        moves = []
        for rr in range(rows):
            for cc in range(cols):
                e = pick(cc, u, cols)
                moves.append((e // per_row * cols + rr * per_row + e % per_row, rr * cols + cc))
        lefts.append(lax.ppermute(flat, ("row", "col"), moves))
    one = k_count * j_count * max(mix, width)
    near = one * (4 * (rows + 2) + 2 * (rows + cols)) <= NEAR_BYTES
    held = pltpu.VMEM if near else jax.ShapeDtypeStruct
    right, gate, left_both = call(
        right_kernel,
        near,
        (held((rows,) + block, F32), held((k_count * j_count, width), F32),
         held((width, 2 * mix), BF16)),
        [], flat, right_weight, right_gate, left_weight, left_gate, out_gate, *rights, loose=6,
    )
    total = None
    _, steps = step_order(rows, cols)
    for u in steps:
        args = [lefts[u], left_both, right]
        if u == steps[0]:
            total = call(functools.partial(first_kernel, u), near, held(block, F32), [block], *args)
        elif u != steps[-1]:
            total = call(
                functools.partial(next_kernel, u), near, held(block, F32), [block],
                *args, total, aliases={3: 0},
            )
        else:
            out = call(
                functools.partial(last_kernel, u, n), near,
                jax.ShapeDtypeStruct(flat.shape, BF16), [block],
                *args, total, gate, mid_gain.reshape(1, -1), out_weight,
            )
    return out.reshape(pair_rows.shape)


def solution(mesh):
    placed = (
        P(("trial", "row"), "col", None),
        P("trial", None),
        P("trial", None),
        P("trial", None),
        P("trial", None),
        P(),
        P("trial", None),
        P("trial", None),
    )
    return jax.shard_map(
        update,
        mesh=mesh,
        in_specs=placed,
        out_specs=P(("trial", "row"), "col", None),
        check_vma=False,
    )
```
